32 devices in a mesh: dom: 16 (over z, y, x), sub: 2 (over core).
Axes of the slice: x: 2, y: 2, z: 4, core: 2. Of those that a mesh axis runs over, the one named last changes fastest.
Arguments:
- rhs: float32 [8192], P(('dom', 'sub')), may hold values from -6 to 6
- diagonal: float32 [8192], P(('dom', 'sub')), may hold values from 1 to 2
- self_raw: float32 [8192, 256], P(('dom', 'sub')), may hold values from -0.046875 to 0.046875
- coupling: float32 [8192, 256], P(('dom', 'sub')), may hold values from -0.046875 to 0.046875
- pattern: int32 [64, 2], P(('dom', 'sub')), may hold values 0 or 1
- prolong: float32 [8192, 128], P(('dom', 'sub')), may hold values from -0.5 to 0.5
- coarse_raw: float32 [4096, 256], P('dom'), may hold values from -0.0234375 to 0.0234375
- coarse_diagonal: float32 [4096], P('dom'), may hold values from 1 to 2
Outputs:
- solution: float32 [8192], P(('dom', 'sub'))
- residual: float32 [8192], P(('dom', 'sub'))
- norms: float32 [3], replicated
The draws below stay inside these ranges and needn't reach their ends.
All inputs are finite; a program needn't handle non-finite values. No bound on the sum of `pattern` on one device may be relied on, other than what follows from the above.
Results may differ from the reference program's by a relative error of at most 0.0003.
Values sent between devices are 32-bit elements; how exact they have to be, the bound alone decides.
No kernel may reach another device: no remote copies, remote signals or barrier semaphores. Data moves between devices by JAX's collectives and lax.ppermute only.
A program may use at most 64 MiB of HBM per device.

```python
import jax
import jax.numpy as jnp
from jax import lax

B = 128
NB = 2
NC = 128
ITERS = 3
DEVS = 32
ROWS = 8192
N_DOM = 16
N_SUB = 2


def place_ends(array, key, low, top_value):
    extent = array.shape
    place = [jax.random.randint(jax.random.fold_in(key, axis), (), 0, extent[axis]) for axis in range(len(extent))]
    array = array.at[tuple(place)].set(low)
    longest = extent.index(max(extent))
    place[longest] = (place[longest] + 1) % extent[longest]
    return array.at[tuple(place)].set(top_value)


def block_levels(own_key, dims, split, least, high):
    loudness, own = 1.0, jax.random.fold_in(own_key, 6)
    for axis_at, shards_of in split:
        heights = jnp.exp(jax.random.uniform(jax.random.fold_in(own, axis_at), (shards_of,), jnp.float32, least / len(split), high / len(split)))
        loudness = loudness * jnp.repeat(heights, dims[axis_at] // shards_of).reshape([-1 if axis == axis_at else 1 for axis in range(len(dims))])
    return loudness


def centred(key, shape, scale, limit, cuts=(), kind=jnp.bfloat16):
    values = scale * jax.random.normal(key, shape, jnp.float32)
    if cuts:
        values = values * block_levels(key, shape, cuts, -0.22, 0.18)
    return jnp.clip(values, -limit, limit).astype(kind)


def setup_inputs(seed: int = 0) -> dict:
    arg_keys = jax.random.split(jax.random.key(seed), 9)
    return {
        "rhs": centred(arg_keys[0], (ROWS,), 1.0, 6.0, ((0, 32),), jnp.float32),
        "diagonal": jnp.clip(1.0 + 1.0 * jax.random.uniform(arg_keys[1], (ROWS,), jnp.float32) ** block_levels(arg_keys[1], (ROWS,), ((0, 32),), -0.2, 0.2), 1.0, 2.0),
        "self_raw": centred(arg_keys[2], (ROWS, NB * B), (NB * B * NB * B // 4) ** -0.5, 0.046875, ((0, 32),), jnp.float32),
        "coupling": centred(arg_keys[3], (ROWS, NB * B), (NB * B * NB * B // 4) ** -0.5, 0.046875, ((0, 32),), jnp.float32),
        "pattern": place_ends((jax.random.randint(arg_keys[4], (DEVS * NB, NB), 0, 3) < 2).astype(jnp.int32), jax.random.fold_in(arg_keys[4], 1), 0, 1),
        "prolong": centred(arg_keys[5], (ROWS, NC), NC ** -0.5, 0.5, ((0, 32),), jnp.float32),
        "coarse_raw": centred(arg_keys[6], (N_DOM * 2 * NC, 2 * NC), (4 * NC * NC) ** -0.5, 0.0234375, ((0, 16),), jnp.float32),
        "coarse_diagonal": jnp.clip(1.0 + 1.0 * jax.random.uniform(arg_keys[7], (N_DOM * 2 * NC,), jnp.float32) ** block_levels(arg_keys[7], (N_DOM * 2 * NC,), ((0, 16),), -0.2, 0.2), 1.0, 2.0),
    }


OMEGA = 0.7
HIGH = lax.Precision.HIGHEST


def reference(rhs, diagonal, self_raw, coupling, pattern, prolong, coarse_raw, coarse_diagonal):
    devs = N_DOM * N_SUB
    width = NB * B
    chips = N_DOM
    eye = jnp.eye(width, dtype=jnp.float32)
    raw = self_raw.reshape(devs, width, width)
    diag = diagonal.reshape(devs, width)
    selfm = 0.5 * (raw + jnp.transpose(raw, (0, 2, 1))) * (1.0 - eye) + eye * diag[:, :, None]
    mask = pattern.reshape(devs, NB, 1, NB, 1).astype(jnp.float32)
    mask = jnp.broadcast_to(mask, (devs, NB, B, NB, B)).reshape(devs, width, width)
    coup = coupling.reshape(devs, width, width) * mask
    dinv = 1.0 / diag
    pro = prolong.reshape(devs, width, NC)
    ceye = jnp.eye(2 * NC, dtype=jnp.float32)
    craw = coarse_raw.reshape(chips, 2 * NC, 2 * NC)
    cdiag = coarse_diagonal.reshape(chips, 2 * NC)
    cmat = 0.5 * (craw + jnp.transpose(craw, (0, 2, 1))) * (1.0 - ceye) + ceye * cdiag[:, :, None]
    cdinv = 1.0 / cdiag
    zero_row = jnp.zeros((1, width), jnp.float32)

    def apply(vec):
        own = jnp.einsum('dij,dj->di', selfm, vec, precision=HIGH)
        nxt = jnp.concatenate([vec[1:], zero_row], axis=0)
        upper = jnp.einsum('dij,dj->di', coup, nxt, precision=HIGH)
        low = jnp.einsum('dji,dj->di', coup, vec, precision=HIGH)
        low = jnp.concatenate([zero_row, low[:-1]], axis=0)
        return own + upper + low

    def precond(wvec):
        first = OMEGA * dinv * wvec
        resid = wvec - apply(first)
        rcoarse = jnp.einsum('dij,di->dj', pro, resid, precision=HIGH).reshape(chips, 2 * NC)
        eone = cdinv * rcoarse
        etwo = eone + cdinv * (rcoarse - jnp.einsum('cij,cj->ci', cmat, eone, precision=HIGH))
        second = first + jnp.einsum('dij,dj->di', pro, etwo.reshape(devs, NC), precision=HIGH)
        return second + OMEGA * dinv * (wvec - apply(second))

    resid = rhs.reshape(devs, width)
    solution = jnp.zeros_like(resid)
    uvec = precond(resid)
    wvec = apply(uvec)
    zeros = jnp.zeros_like(resid)
    pvec, svec, qvec, zvec = zeros, zeros, zeros, zeros
    gamma_prev = jnp.float32(1.0)
    alpha_prev = jnp.float32(1.0)
    norm_list = []
    for step in range(ITERS):
        gamma = jnp.sum(resid * uvec)
        delta = jnp.sum(wvec * uvec)
        norm_list.append(jnp.sum(resid * resid))
        mvec = precond(wvec)
        nvec = apply(mvec)
        if step == 0:
            beta = jnp.float32(0.0)
            alpha = gamma / delta
        else:
            beta = gamma / gamma_prev
            alpha = gamma / (delta - beta * gamma / alpha_prev)
        zvec = nvec + beta * zvec
        qvec = mvec + beta * qvec
        svec = wvec + beta * svec
        pvec = uvec + beta * pvec
        solution = solution + alpha * pvec
        resid = resid - alpha * svec
        uvec = uvec - alpha * qvec
        wvec = wvec - alpha * zvec
        gamma_prev = gamma
        alpha_prev = alpha
    return solution.reshape(-1), resid.reshape(-1), jnp.stack(norm_list)
```

```python
import jax
import jax.numpy as jnp
from jax import lax
from jax.sharding import PartitionSpec as P

ITERS = 3


OMEGA = 0.7
HIGH = lax.Precision.HIGHEST


def passed_along(value, axis, steps):
    count = lax.axis_size(axis)
    initial, last = (max(0, -steps), min(count, count - steps))
    return lax.ppermute(value, axis, [(source, source + steps) for source in range(initial, last)])


def three_sums(resid, uvec, wvec):
    axes = ("dom", "sub")
    count = lax.axis_size(axes)
    parts = jnp.stack([jnp.sum(resid * uvec), jnp.sum(wvec * uvec), jnp.sum(resid * resid)])
    sent = jnp.broadcast_to(jnp.pad(parts, (0, 125))[None], (count, 128))
    got = lax.all_to_all(sent, axes, 0, 0, tiled=True)
    sums = jnp.sum(got, axis=0)
    return sums[0], sums[1], sums[2]


def per_device(rhs, diagonal, self_raw, coupling, pattern, prolong, coarse_raw, coarse_diagonal):
    width = rhs.shape[0]
    blocks = pattern.shape[0]
    block_rows = width // blocks
    coarse = prolong.shape[1]
    eye = jnp.eye(width, dtype=jnp.float32)
    selfm = 0.5 * (self_raw + self_raw.T) * (1.0 - eye) + eye * diagonal[:, None]
    mask = pattern.reshape(blocks, 1, blocks, 1).astype(jnp.float32)
    mask = jnp.broadcast_to(mask, (blocks, block_rows, blocks, block_rows)).reshape(width, width)
    coup = coupling * mask
    dinv = 1.0 / diagonal
    ceye = jnp.eye(2 * coarse, dtype=jnp.float32)
    cmat = 0.5 * (coarse_raw + coarse_raw.T) * (1.0 - ceye) + ceye * coarse_diagonal[:, None]
    cdinv = 1.0 / coarse_diagonal
    offset = lax.axis_index("sub") * coarse

    def apply(vec):
        upper = passed_along(vec, ("dom", "sub"), -1)
        lower = passed_along(jnp.dot(vec, coup, precision=HIGH), ("dom", "sub"), 1)
        return jnp.dot(selfm, vec, precision=HIGH) + jnp.dot(coup, upper, precision=HIGH) + lower

    def precond(wvec):
        first = OMEGA * dinv * wvec
        resid = wvec - apply(first)
        rcoarse = jnp.dot(resid, prolong, precision=HIGH)
        own_inv = lax.dynamic_slice_in_dim(cdinv, offset, coarse, 0)
        own_rows = lax.dynamic_slice_in_dim(cmat, offset, coarse, 0)
        eone = own_inv * rcoarse
        eboth = lax.all_gather(eone, "sub", axis=0, tiled=True)
        mine = eone + own_inv * (rcoarse - jnp.dot(own_rows, eboth, precision=HIGH))
        second = first + jnp.dot(prolong, mine, precision=HIGH)
        return second + OMEGA * dinv * (wvec - apply(second))

    resid = rhs
    solution = jnp.zeros_like(rhs)
    uvec = precond(resid)
    wvec = apply(uvec)
    zeros = jnp.zeros_like(rhs)
    pvec, svec, qvec, zvec = (zeros, zeros, zeros, zeros)
    gamma_prev = jnp.float32(1.0)
    alpha_prev = jnp.float32(1.0)
    norm_list = []
    for step in range(ITERS):
        mvec = precond(wvec)
        nvec = apply(mvec)
        gamma, delta, rnorm = three_sums(resid, uvec, wvec)
        norm_list.append(rnorm)
        if step == 0:
            beta = jnp.float32(0.0)
            alpha = gamma / delta
        else:
            beta = gamma / gamma_prev
            alpha = gamma / (delta - beta * gamma / alpha_prev)
        zvec = nvec + beta * zvec
        qvec = mvec + beta * qvec
        svec = wvec + beta * svec
        pvec = uvec + beta * pvec
        solution = solution + alpha * pvec
        resid = resid - alpha * svec
        uvec = uvec - alpha * qvec
        wvec = wvec - alpha * zvec
        gamma_prev = gamma
        alpha_prev = alpha
    return (solution, resid, jnp.stack(norm_list))


def solution(mesh):
    in_specs = (
        P(("dom", "sub")),
        P(("dom", "sub")),
        P(("dom", "sub"), None),
        P(("dom", "sub"), None),
        P(("dom", "sub"), None),
        P(("dom", "sub"), None),
        P("dom", None),
        P("dom"),
    )
    out_specs = (P(("dom", "sub")), P(("dom", "sub")), P())
    return jax.shard_map(
        per_device, mesh=mesh, in_specs=in_specs, out_specs=out_specs, check_vma=False
    )
```

```python
import functools

import jax
import jax.numpy as jnp
from jax import lax
from jax.experimental import pallas as pl
from jax.experimental.pallas import tpu as pltpu
from jax.sharding import PartitionSpec as P

AXES = ("dom", "sub")
OMEGA = 0.7
LANES = 128
GROUP = 16
F32 = jnp.float32


def local_call(body, outs, *args, smem=(), scratch=(), flops=200_000):
    spaces = [pltpu.SMEM if i in smem else pltpu.VMEM for i in range(len(args))]
    return pl.pallas_call(
        body,
        out_shape=[jax.ShapeDtypeStruct(s, F32) for s in outs],
        in_specs=[pl.BlockSpec(memory_space=s) for s in spaces],
        out_specs=[pl.BlockSpec(memory_space=pltpu.VMEM) for _ in outs],
        scratch_shapes=list(scratch),
        cost_estimate=pl.CostEstimate(flops=flops, bytes_accessed=1000, transcendentals=0),
        compiler_params=pltpu.CompilerParams(vmem_limit_bytes=8 * 1024 * 1024),
    )(*args)


def unit(rows, cols):
    shape = (rows, cols)
    return lax.broadcasted_iota(jnp.int32, shape, 0) == lax.broadcasted_iota(jnp.int32, shape, 1)


def over_lanes(a):
    return jnp.sum(a, axis=1, keepdims=True)


def over_rows(a):
    return jnp.sum(a, axis=0, keepdims=True)


def as_row(col):
    eye = unit(LANES, LANES)
    pieces = [
        over_rows(jnp.where(eye, col[k : k + LANES], 0.0)) for k in range(0, col.shape[0], LANES)
    ]
    return jnp.concatenate(pieces, axis=1)


def as_col(row):
    eye = unit(LANES, LANES)
    pieces = [
        over_lanes(jnp.where(eye, row[:, k : k + LANES], 0.0))
        for k in range(0, row.shape[1], LANES)
    ]
    return jnp.concatenate(pieces, axis=0)


def two_sum(a, b):
    s = a + b
    t = s - a
    return s, (a - (s - t)) + (b - t)


def halves(a):
    t = 4097.0 * a
    hi = t - (t - a)
    return hi, a - hi


def two_prod(a, b):
    p = a * b
    ah, al = halves(a)
    bh, bl = halves(b)
    return p, ((ah * bh - p) + ah * bl + al * bh) + al * bl


def pair_add(a, b):
    s, e = two_sum(a[0], b[0])
    e = e + (a[1] + b[1])
    hi = s + e
    return hi, e - (hi - s)


def pair_mul(a, b):
    p, e = two_prod(a[0], b[0])
    e = e + (a[0] * b[1] + a[1] * b[0])
    hi = p + e
    return hi, e - (hi - p)


def start_body(rhs, diag, coup, pattern, cm, sent):
    blocks = pattern.shape[0]
    step = coup.shape[0] // blocks
    for i in range(blocks):
        for j in range(blocks):
            keep = pattern[i, j].astype(F32)
            rows, cols = pl.ds(i * step, step), pl.ds(j * step, step)
            cm[rows, cols] = coup[rows, cols] * keep
    scale = OMEGA / diag[...]
    first = scale * rhs[...]
    sent[0:1] = over_rows(cm[...] * as_col(first))
    sent[1:2] = first
    sent[2:3] = scale


def setup_body(raw, diag, craw, cdiag, pro, cm, packed, fmat):
    width = raw.shape[0]
    coarse = pro.shape[1]
    eye = unit(width, width)
    r = raw[...]
    packed[0:width] = jnp.where(eye, diag[...] * (1.0 - 1.0 / OMEGA), 0.5 * (r + r.T))
    packed[width : 2 * width] = cm[...]
    packed[2 * width :] = pro[...].T
    q = craw[...]
    inv = 1.0 / cdiag[...]
    full = jnp.where(unit(2 * coarse, 2 * coarse), inv, -0.5 * (q + q.T) * inv * as_col(inv))
    core = lax.axis_index("sub")

    @pl.when(core == 0)
    def _():
        fmat[...] = full

    @pl.when(core != 0)
    def _():
        swapped = jnp.concatenate([full[coarse:], full[:coarse]], axis=0)
        fmat[...] = jnp.concatenate([swapped[:, coarse:], swapped[:, :coarse]], axis=1)


def inner_edge_body(packed, got, ein, eint):
    width = ein.shape[0]
    core = lax.axis_index("sub")

    @pl.when(core == 0)
    def _():
        c = packed[width : 2 * width]
        ein[...] = c
        eint[...] = c.T

    @pl.when(core != 0)
    def _():
        c = got[width : 2 * width]
        ein[...] = c.T
        eint[...] = c


def outer_edge_body(cm, got, eout, eoutt):
    core = lax.axis_index("sub")

    @pl.when(core == 0)
    def _():
        c = got[...]
        eout[...] = c.T
        eoutt[...] = c

    @pl.when(core != 0)
    def _():
        c = cm[...]
        eout[...] = c
        eoutt[...] = c.T


def restrict_first_body(sent, inner, outer, packed, cm, pro, out):
    width = sent.shape[1]
    zero = lax.axis_index("sub") == 0
    raw = jnp.where(zero, inner[1:2], outer[1:2])
    done = jnp.where(zero, outer[0:1], inner[0:1])
    r = over_lanes(
        packed[0:width] * sent[1:2] + cm[...] * raw + jnp.where(unit(width, width), done, 0.0)
    )
    out[...] = -over_rows(pro[...] * r)


def restrict_local_body(state, packed, ein, pro, out):
    width = state.shape[1]
    r = over_lanes(packed[0:width] * state[1:2] + ein[...] * state[2:3])
    out[...] = over_rows(pro[...] * r)


def restrict_body(local, x1o, eout, pro, out):
    r = over_lanes(eout[...] * x1o[...])
    out[...] = -(local[...] + over_rows(pro[...] * r))


def coarse_body(ca, cb, state, fmat, packed, other, ein, scale, out):
    width = state.shape[1]
    coarse = ca.shape[1]
    both = jnp.concatenate([ca[...], cb[...]], axis=1)
    e = over_lanes(fmat[...] * both)
    xa = state[1:2] + over_rows(packed[2 * width :] * e[:coarse])
    xb = state[2:3] + over_rows(other[2 * width :] * e[coarse:])
    v = over_lanes(packed[0:width] * xa + ein[...] * xb)
    out[0:1] = xa
    out[1:2] = scale[0:1] * (state[0:1] - as_row(v))


def edge_local_body(sent, eoutt, scale, out):
    out[...] = scale[2:3] * as_row(over_lanes(eoutt[...] * sent[0:1]))


def edge_body(sent, got, own, eout, scale, out):
    u = as_row(over_lanes(eout[...] * got[0:1]))
    mo = got[1:2] - own[...]
    out[0:1] = sent[1:2] - scale[0:1] * u
    out[1:2] = as_row(over_lanes(eout[...] * mo))


def apply_body(sent, got, packed, other, ein, eint, scale, state, x1):
    width = sent.shape[1]
    ma, mb = sent[0:1], got[0:1]
    va = over_lanes(packed[0:width] * ma + ein[...] * mb)
    vb = over_lanes(other[0:width] * mb + eint[...] * ma)
    na = as_row(va) + sent[1:2] + ma / scale[0:1]
    nb = as_row(vb) + got[1:2] + mb / scale[1:2]
    xa = scale[0:1] * na
    state[0:1] = na
    state[1:2] = xa
    state[2:3] = scale[1:2] * nb
    x1[...] = xa


def scale_body(sent, inner, outer, rhs, scale, state):
    scale[0:1] = sent[2:3]
    scale[1:2] = inner[2:3]
    scale[2:3] = outer[2:3]
    state[0:1] = rhs[...]
    state[1:2] = sent[1:2]
    state[2:3] = inner[1:2]


def gram_body(*refs):
    lefts, rights, out, xs, ys = refs[:4], refs[4:7], refs[7], refs[8], refs[9]
    xs[...] = jnp.zeros_like(xs)
    ys[...] = jnp.zeros_like(ys)
    for i in range(3):
        for j in range(3):
            for group, a, b in (
                (0, lefts[i], rights[j]),
                (1, lefts[i + 1], rights[j]),
                (2, lefts[i], lefts[j]),
            ):
                at = group * GROUP + 3 * i + j
                xs[at : at + 1] = a[0:1]
                ys[at : at + 1] = b[0:1]
    hi, lo = two_prod(xs[...], ys[...])
    parts = [(hi[:, k : k + LANES], lo[:, k : k + LANES]) for k in range(0, hi.shape[1], LANES)]
    total = functools.reduce(pair_add, parts)
    step = LANES // 2
    while step:
        total = pair_add(total, tuple(pltpu.roll(t, step, 1) for t in total))
        step //= 2
    eye = unit(xs.shape[0], LANES)
    hi, lo = (over_rows(jnp.where(eye, t, 0.0)) for t in total)
    row = hi + pltpu.roll(jnp.broadcast_to(lo, (8, LANES)), LANES // 2, 1)[0:1]
    out[...] = jnp.broadcast_to(row, out.shape)


def finish_body(got, b, w0, n0, n1, u0, m0, m1, sol, res, norms):
    full = got[...]
    rows = full.shape[0]
    tiles = [full[k : k + 8] for k in range(0, rows, 8)]
    pairs = [(t, pltpu.roll(t, LANES // 2, 1)) for t in tiles]
    while len(pairs) > 1:
        rest = pairs[len(pairs) // 2 * 2 :]
        pairs = [pair_add(pairs[k], pairs[k + 1]) for k in range(0, len(pairs) - 1, 2)] + rest
    gram = pairs[0]
    for step in (4, 2, 1):
        gram = pair_add(gram, tuple(pltpu.roll(t, step, 0) for t in gram))
    lane = lax.broadcasted_iota(jnp.int32, (8, LANES), 1)
    term = lane % GROUP
    left, right = term // 3, term % 3
    valid = (term < 9) & (lane < 3 * GROUP)
    gram = tuple(jnp.where(valid, t, 0.0) for t in gram)

    def at(value, where):
        return over_lanes(jnp.where(lane == where, value, 0.0))

    def form(c1, c2):
        def coefficient(index):
            hi = jnp.where(index == 0, 1.0, jnp.where(index == 1, -c1[0], c2[0]))
            lo = jnp.where(index == 0, 0.0, jnp.where(index == 1, -c1[1], c2[1]))
            return hi, lo

        total = pair_mul(pair_mul(coefficient(left), coefficient(right)), gram)
        for step in (8, 4, 2, 1):
            total = pair_add(total, tuple(pltpu.roll(t, LANES - step, 1) for t in total))
        return tuple(at(total[0], g * GROUP) for g in range(3))

    gamma0, delta0, rho0 = (at(gram[0], g * GROUP) for g in range(3))
    zero = jnp.zeros_like(gamma0)
    alpha0 = gamma0 / delta0
    gamma1, delta1, rho1 = form((alpha0, zero), (zero, zero))
    beta1 = gamma1 / gamma0
    alpha1 = gamma1 / (delta1 - beta1 * gamma1 / alpha0)
    c1 = pair_add((alpha0, zero), pair_mul((alpha1, zero), two_sum(zero + 1.0, beta1)))
    gamma2, delta2, rho2 = form(c1, two_prod(alpha0, alpha1))
    beta2 = gamma2 / gamma1
    alpha2 = gamma2 / (delta2 - beta2 * gamma2 / alpha1)

    a0, a1, a2, b1, b2 = (t[0:1] for t in (alpha0, alpha1, alpha2, beta1, beta2))
    rb, rw0, rn0, rn1, ru0, rm0, rm1 = (t[0:1] for t in (b, w0, n0, n1, u0, m0, m1))
    r1 = rb - a0 * rw0
    u1 = ru0 - a0 * rm0
    w1 = rw0 - a0 * rn0
    s1 = w1 + b1 * rw0
    p1 = u1 + b1 * ru0
    z1 = (rn0 - a0 * rn1) + b1 * rn0
    q1 = (rm0 - a0 * rm1) + b1 * rm0
    r2 = r1 - a1 * s1
    u2 = u1 - a1 * q1
    w2 = w1 - a1 * z1
    s2 = w2 + b2 * s1
    p2 = u2 + b2 * p1
    sol[...] = a0 * ru0 + a1 * p1 + a2 * p2
    res[...] = r2 - a2 * s2
    where = lane[0:1]
    row = jnp.where(where == 0, rho0[0:1], jnp.where(where == 1, rho1[0:1], rho2[0:1]))
    norms[...] = row[:, :3]


def per_device(rhs, diagonal, self_raw, coupling, pattern, prolong, coarse_raw, coarse_diagonal):
    width, coarse = rhs.shape[0], prolong.shape[1]
    chips = lax.axis_size("dom")
    inner = [(2 * g + c, 2 * g + 1 - c) for g in range(chips) for c in range(2)]
    up = [(2 * g + 1, 2 * g + 2) for g in range(chips - 1)]
    outer = up + [(b, a) for a, b in up]
    square, row = (width, width), (1, width)

    def move(value, pairs):
        return lax.ppermute(value, AXES, pairs)

    rhs_row, diag_row = rhs.reshape(row), diagonal.reshape(row)
    cm, sent = local_call(
        start_body, [square, (3, width)], rhs_row, diag_row, coupling, pattern, smem=(3,)
    )
    from_outer = move(sent, outer)
    from_inner = move(sent, inner)
    packed, fmat = local_call(
        setup_body,
        [(2 * width + coarse, width), (2 * coarse, 2 * coarse)],
        self_raw,
        diag_row,
        coarse_raw,
        coarse_diagonal.reshape(1, 2 * coarse),
        prolong,
        cm,
        flops=1_000_000,
    )
    other = move(packed, inner)
    cm_up = move(cm, up)
    scale, state = local_call(
        scale_body, [(3, width), (3, width)], sent, from_inner, from_outer, rhs_row
    )
    c_own = local_call(
        restrict_first_body, [(1, coarse)], sent, from_inner, from_outer, packed, cm, prolong
    )[0]
    ein, eint = local_call(inner_edge_body, [square, square], packed, other)
    eout, eoutt = local_call(outer_edge_body, [square, square], cm, cm_up)

    lefts, rights = [rhs_row], []
    for cycle in range(3):
        if cycle:
            x1o = move(x1, outer)
            local = local_call(restrict_local_body, [(1, coarse)], state, packed, ein, prolong)[0]
            c_own = local_call(restrict_body, [(1, coarse)], local, x1o, eout, prolong)[0]
        c_other = move(c_own, inner)
        half = local_call(
            coarse_body, [(2, width)], c_own, c_other, state, fmat, packed, other, ein, scale
        )[0]
        got = move(half, outer)
        own = local_call(edge_local_body, [row], half, eoutt, scale)[0]
        mt = local_call(edge_body, [(2, width)], half, got, own, eout, scale)[0]
        mt_other = move(mt, inner)
        state, x1 = local_call(
            apply_body, [(3, width), row], mt, mt_other, packed, other, ein, eint, scale
        )
        lefts.append(state)
        rights.append(mt)

    count = 2 * chips
    parts = local_call(
        gram_body,
        [(count, LANES)],
        *lefts,
        *rights,
        scratch=[pltpu.VMEM((3 * GROUP, width), F32)] * 2,
    )[0]
    sums = lax.all_to_all(parts, AXES, 0, 0, tiled=True)
    sums = jnp.pad(sums, ((0, -count % 8), (0, 0)))
    sol, res, norms = local_call(finish_body, [row, row, (1, 3)], sums, *lefts, *rights)
    return sol.reshape(width), res.reshape(width), norms.reshape(3)


def solution(mesh):
    assert mesh.shape["sub"] == 2
    both = P(AXES)
    wide = P(AXES, None)
    return jax.shard_map(
        per_device,
        mesh=mesh,
        in_specs=(both, both, wide, wide, wide, wide, P("dom", None), P("dom")),
        out_specs=(both, both, P()),
        check_vma=False,
    )
```

```python
import functools

import jax
import jax.numpy as jnp
from jax import lax
from jax.experimental import pallas as pl
from jax.experimental.pallas import tpu as pltpu
from jax.sharding import PartitionSpec as P

AXES = ("dom", "sub")
OMEGA = 0.7
LANES = 128
GROUP = 16
F32 = jnp.float32


def local_call(body, outs, *args, hbm=0, scratch=(), flops=200_000):
    spaces = [pltpu.HBM if i < hbm else pltpu.VMEM for i in range(len(args))]
    args = [pltpu.with_memory_space_constraint(a, pltpu.HBM) for a in args[:hbm]] + list(args[hbm:])
    return pl.pallas_call(
        body,
        out_shape=[jax.ShapeDtypeStruct(s, F32) for s in outs],
        in_specs=[pl.BlockSpec(memory_space=s) for s in spaces],
        out_specs=[pl.BlockSpec(memory_space=pltpu.VMEM) for _ in outs],
        scratch_shapes=list(scratch),
        cost_estimate=pl.CostEstimate(flops=flops, bytes_accessed=1000, transcendentals=0),
        compiler_params=pltpu.CompilerParams(vmem_limit_bytes=8 * 1024 * 1024),
    )(*args)


def unit(rows, cols):
    shape = (rows, cols)
    return lax.broadcasted_iota(jnp.int32, shape, 0) == lax.broadcasted_iota(jnp.int32, shape, 1)


def over_lanes(a):
    return jnp.sum(a, axis=1, keepdims=True)


def over_rows(a):
    return jnp.sum(a, axis=0, keepdims=True)


def as_row(col):
    eye = unit(LANES, LANES)
    pieces = [
        over_rows(jnp.where(eye, col[k : k + LANES], 0.0)) for k in range(0, col.shape[0], LANES)
    ]
    return jnp.concatenate(pieces, axis=1)


def as_col(row):
    eye = unit(LANES, LANES)
    pieces = [
        over_lanes(jnp.where(eye, row[:, k : k + LANES], 0.0))
        for k in range(0, row.shape[1], LANES)
    ]
    return jnp.concatenate(pieces, axis=0)


def two_sum(a, b):
    s = a + b
    t = s - a
    return s, (a - (s - t)) + (b - t)


def halves(a):
    t = 4097.0 * a
    hi = t - (t - a)
    return hi, a - hi


def two_prod(a, b):
    p = a * b
    ah, al = halves(a)
    bh, bl = halves(b)
    return p, ((ah * bh - p) + ah * bl + al * bh) + al * bl


def pair_add(a, b):
    s, e = two_sum(a[0], b[0])
    e = e + (a[1] + b[1])
    hi = s + e
    return hi, e - (hi - s)


def pair_mul(a, b):
    p, e = two_prod(a[0], b[0])
    e = e + (a[0] * b[1] + a[1] * b[0])
    hi = p + e
    return hi, e - (hi - p)


def fetch(sources, targets, sems):
    copies = [pltpu.make_async_copy(*pair, sems.at[k]) for k, pair in enumerate(zip(sources, targets))]
    for copy in copies:
        copy.start()
    return copies


def start_body(rhs_h, diag_h, pattern_h, coup_h, cm, sent, rhs, diag, pattern, coup, sems):
    for copy in fetch((rhs_h, diag_h, pattern_h, coup_h), (rhs, diag, pattern, coup), sems):
        copy.wait()
    blocks = pattern.shape[0]
    step = coup.shape[0] // blocks
    for i in range(blocks):
        for j in range(blocks):
            keep = pattern[i : i + 1, j : j + 1].astype(F32)
            rows, cols = pl.ds(i * step, step), pl.ds(j * step, step)
            cm[rows, cols] = coup[rows, cols] * keep
    scale = OMEGA / diag[...]
    first = scale * rhs[...]
    sent[0:1] = over_rows(cm[...] * as_col(first))
    sent[1:2] = first
    sent[2:3] = scale
    sent[3:4] = rhs[...]


def setup_body(
    raw_h, craw_h, cdiag_h, pro_h, sent, cm, packed, fmat, raw, craw, cdiag, pro, sems
):
    width = raw.shape[0]
    coarse = pro.shape[1]
    copies = fetch((raw_h, pro_h, cdiag_h, craw_h), (raw, pro, cdiag, craw), sems)
    packed[width : 2 * width] = cm[...]
    eye = unit(width, width)
    diag = OMEGA / sent[2:3]
    copies[0].wait()
    r = raw[...]
    packed[0:width] = jnp.where(eye, diag * (1.0 - 1.0 / OMEGA), 0.5 * (r + r.T))
    copies[1].wait()
    packed[2 * width :] = pro[...].T
    copies[2].wait()
    copies[3].wait()
    q = craw[...]
    inv = 1.0 / cdiag[...]
    fmat[...] = jnp.where(
        unit(2 * coarse, 2 * coarse), inv, -0.5 * (q + q.T) * inv * as_col(inv)
    )


def parity():
    return lax.axis_index("dom") % 2


def both_ways(even, odd, rightward, leftward):
    is_even = parity() == 0
    even[...] = jnp.where(is_even, rightward, leftward)
    odd[...] = jnp.where(is_even, leftward, rightward)


def from_sides(even, odd):
    dom, last = lax.axis_index("dom"), lax.axis_size("dom") - 1
    is_even = parity() == 0
    e, o = even[...], odd[...]
    left = jnp.where(dom > 0, jnp.where(is_even, o, e), 0.0)
    right = jnp.where(dom < last, jnp.where(is_even, e, o), 0.0)
    return left, right


def pair_body(sent, inner, even, odd, scale, state):
    low = lax.axis_index("sub") == 0
    own, other = sent[...], inner[...]
    left, right = jnp.where(low, own, other), jnp.where(low, other, own)
    both_ways(
        even,
        odd,
        jnp.concatenate([right[0:1], right[2:3]], axis=0),
        left[1:3],
    )
    scale[0:1] = left[2:3]
    scale[1:2] = right[2:3]
    state[0:1] = left[3:4]
    state[1:2] = right[3:4]
    state[2:3] = left[1:2]
    state[3:4] = right[1:2]


def order_body(packed, other, sl, sr, cin, cint, cr, crt, ptl, ptr, prl, prr):
    width = sl.shape[0]

    def place(low, high):
        sl[...] = low[0:width]
        sr[...] = high[0:width]
        c = low[width : 2 * width]
        cin[...] = c
        cint[...] = c.T
        c = high[width : 2 * width]
        cr[...] = c
        crt[...] = c.T
        p = low[2 * width :]
        ptl[...] = p
        prl[...] = p.T
        p = high[2 * width :]
        ptr[...] = p
        prr[...] = p.T

    core = lax.axis_index("sub")

    @pl.when(core == 0)
    def _():
        place(packed, other)

    @pl.when(core != 0)
    def _():
        place(other, packed)


def left_edge_body(up, swapped, cl, clt):
    c = jnp.where(lax.axis_index("sub") == 0, up[...], swapped[...])
    c = jnp.where(lax.axis_index("dom") > 0, c, 0.0)
    cl[...] = c.T
    clt[...] = c


def smooth(c, state, scale, fmat, sl, sr, cin, cint, ptl, ptr, half, even, odd):
    coarse = ptl.shape[0]
    e = over_lanes(fmat[...] * c)
    xl = state[2:3] + over_rows(ptl[...] * e[:coarse])
    xr = state[3:4] + over_rows(ptr[...] * e[coarse:])
    vl = as_row(over_lanes(sl[...] * xl + cin[...] * xr))
    vr = as_row(over_lanes(sr[...] * xr + cint[...] * xl))
    ml = scale[0:1] * (state[0:1] - vl)
    mr = scale[1:2] * (state[1:2] - vr)
    half[0:1] = xl
    half[1:2] = xr
    half[2:3] = ml
    half[3:4] = mr
    both_ways(
        even, odd, jnp.concatenate([xr, mr], axis=0), jnp.concatenate([xl, ml], axis=0)
    )


def first_body(
    goteven, gotodd, state, scale, fmat, sl, sr, cin, cint, cr, ptl, ptr, prl, prr, half, even, odd, outer
):
    width = sl.shape[0]
    left, right = from_sides(goteven, gotodd)
    outer[0:1] = left[1:2]
    outer[1:2] = right[1:2]
    x1l, x1r = state[2:3], state[3:4]
    done = jnp.where(unit(width, width), left[0:1], 0.0)
    rl = over_lanes(sl[...] * x1l + cin[...] * x1r + done)
    rr = over_lanes(sr[...] * x1r + cint[...] * x1l + cr[...] * right[0:1])
    c = jnp.concatenate([over_rows(prl[...] * rl), over_rows(prr[...] * rr)], axis=1)
    smooth(-c, state, scale, fmat, sl, sr, cin, cint, ptl, ptr, half, even, odd)


def restrict_local_body(state, sl, sr, cin, cint, prl, prr, out):
    x1l, x1r = state[2:3], state[3:4]
    rl = over_lanes(sl[...] * x1l + cin[...] * x1r)
    rr = over_lanes(sr[...] * x1r + cint[...] * x1l)
    out[...] = jnp.concatenate([over_rows(prl[...] * rl), over_rows(prr[...] * rr)], axis=1)


def next_body(
    goteven, gotodd, local, state, scale, fmat, sl, sr, cin, cint, cl, cr, ptl, ptr, prl, prr, half, even, odd
):
    left, right = from_sides(goteven, gotodd)
    rl = over_lanes(cl[...] * left)
    rr = over_lanes(cr[...] * right)
    c = jnp.concatenate([over_rows(prl[...] * rl), over_rows(prr[...] * rr)], axis=1)
    smooth(-(local[...] + c), state, scale, fmat, sl, sr, cin, cint, ptl, ptr, half, even, odd)


def edge_local_body(half, outer, clt, crt, out):
    out[0:1] = outer[0:1] * as_row(over_lanes(clt[...] * half[0:1]))
    out[1:2] = outer[1:2] * as_row(over_lanes(crt[...] * half[1:2]))


def apply_body(
    goteven, gotodd, half, owed, scale, sl, sr, cin, cint, cl, cr, state, even, odd, own
):
    left, right = from_sides(goteven, gotodd)
    ml = half[2:3] - scale[0:1] * as_row(over_lanes(cl[...] * left[0:1]))
    mr = half[3:4] - scale[1:2] * as_row(over_lanes(cr[...] * right[0:1]))
    mol = left[1:2] - owed[0:1]
    mor = right[1:2] - owed[1:2]
    nl = as_row(over_lanes(sl[...] * ml + cin[...] * mr + cl[...] * mol)) + ml / scale[0:1]
    nr = as_row(over_lanes(sr[...] * mr + cint[...] * ml + cr[...] * mor)) + mr / scale[1:2]
    xl, xr = scale[0:1] * nl, scale[1:2] * nr
    state[0:1] = nl
    state[1:2] = nr
    state[2:3] = xl
    state[3:4] = xr
    both_ways(even, odd, xr, xl)
    low = lax.axis_index("sub") == 0
    own[0:1] = jnp.where(low, nl, nr)
    own[1:2] = jnp.where(low, ml, mr)


def basis(sent, *owns):
    return [sent[3:4]] + [own[0:1] for own in owns], [own[1:2] for own in owns]


def gram_body(sent, own0, own1, own2, out, xs, ys):
    lefts, rights = basis(sent, own0, own1, own2)
    xs[...] = jnp.zeros_like(xs)
    ys[...] = jnp.zeros_like(ys)
    for i in range(3):
        for j in range(3):
            for group, a, b in (
                (0, lefts[i], rights[j]),
                (1, lefts[i + 1], rights[j]),
                (2, lefts[i], lefts[j]),
            ):
                at = group * GROUP + 3 * i + j
                xs[at : at + 1] = a
                ys[at : at + 1] = b
    hi, lo = two_prod(xs[...], ys[...])
    parts = [(hi[:, k : k + LANES], lo[:, k : k + LANES]) for k in range(0, hi.shape[1], LANES)]
    total = functools.reduce(pair_add, parts)
    step = LANES // 2
    while step:
        total = pair_add(total, tuple(pltpu.roll(t, step, 1) for t in total))
        step //= 2
    eye = unit(xs.shape[0], LANES)
    hi, lo = (over_rows(jnp.where(eye, t, 0.0)) for t in total)
    row = hi + pltpu.roll(jnp.broadcast_to(lo, (8, LANES)), LANES // 2, 1)[0:1]
    out[...] = jnp.broadcast_to(row, out.shape)


def finish_body(got, sent, own0, own1, own2, sol, res, norms):
    full = got[...]
    rows = full.shape[0]
    tiles = [full[k : k + 8] for k in range(0, rows, 8)]
    pairs = [(t, pltpu.roll(t, LANES // 2, 1)) for t in tiles]
    while len(pairs) > 1:
        rest = pairs[len(pairs) // 2 * 2 :]
        pairs = [pair_add(pairs[k], pairs[k + 1]) for k in range(0, len(pairs) - 1, 2)] + rest
    gram = pairs[0]
    for step in (4, 2, 1):
        gram = pair_add(gram, tuple(pltpu.roll(t, step, 0) for t in gram))
    lane = lax.broadcasted_iota(jnp.int32, (8, LANES), 1)
    term = lane % GROUP
    left, right = term // 3, term % 3
    valid = (term < 9) & (lane < 3 * GROUP)
    gram = tuple(jnp.where(valid, t, 0.0) for t in gram)

    def at(value, where):
        return over_lanes(jnp.where(lane == where, value, 0.0))

    def form(c1, c2):
        def coefficient(index):
            hi = jnp.where(index == 0, 1.0, jnp.where(index == 1, -c1[0], c2[0]))
            lo = jnp.where(index == 0, 0.0, jnp.where(index == 1, -c1[1], c2[1]))
            return hi, lo

        total = pair_mul(pair_mul(coefficient(left), coefficient(right)), gram)
        for step in (8, 4, 2, 1):
            total = pair_add(total, tuple(pltpu.roll(t, LANES - step, 1) for t in total))
        return tuple(at(total[0], g * GROUP) for g in range(3))

    gamma0, delta0, rho0 = (at(gram[0], g * GROUP) for g in range(3))
    zero = jnp.zeros_like(gamma0)
    alpha0 = gamma0 / delta0
    gamma1, delta1, rho1 = form((alpha0, zero), (zero, zero))
    beta1 = gamma1 / gamma0
    alpha1 = gamma1 / (delta1 - beta1 * gamma1 / alpha0)
    c1 = pair_add((alpha0, zero), pair_mul((alpha1, zero), two_sum(zero + 1.0, beta1)))
    gamma2, delta2, rho2 = form(c1, two_prod(alpha0, alpha1))
    beta2 = gamma2 / gamma1
    alpha2 = gamma2 / (delta2 - beta2 * gamma2 / alpha1)

    a0, a1, a2, b1, b2 = (t[0:1] for t in (alpha0, alpha1, alpha2, beta1, beta2))
    (rb, rw0, rn0, rn1), (ru0, rm0, rm1) = basis(sent, own0, own1, own2)
    r1 = rb - a0 * rw0
    u1 = ru0 - a0 * rm0
    w1 = rw0 - a0 * rn0
    s1 = w1 + b1 * rw0
    p1 = u1 + b1 * ru0
    z1 = (rn0 - a0 * rn1) + b1 * rn0
    q1 = (rm0 - a0 * rm1) + b1 * rm0
    r2 = r1 - a1 * s1
    u2 = u1 - a1 * q1
    w2 = w1 - a1 * z1
    s2 = w2 + b2 * s1
    p2 = u2 + b2 * p1
    sol[...] = a0 * ru0 + a1 * p1 + a2 * p2
    res[...] = r2 - a2 * s2
    where = lane[0:1]
    row = jnp.where(where == 0, rho0[0:1], jnp.where(where == 1, rho1[0:1], rho2[0:1]))
    norms[...] = row[:, :3]


def exchange_pairs(chips, first):
    pairs = [(2 * g + 1, 2 * g + 2) for g in range(first, chips - 1, 2)]
    used = {p for pair in pairs for p in pair}
    idle = [p for p in range(2 * chips) if p not in used]
    pairs += [(idle[k], idle[k + 1]) for k in range(0, len(idle), 2)]
    return pairs + [(b, a) for a, b in pairs]


def vmem(*shape, dtype=F32):
    return pltpu.VMEM(shape, dtype)


def per_device(rhs, diagonal, self_raw, coupling, pattern, prolong, coarse_raw, coarse_diagonal):
    width, coarse = rhs.shape[0], prolong.shape[1]
    chips = lax.axis_size("dom")
    count = 2 * chips
    inner = [(p, p + 1 - 2 * (p % 2)) for p in range(count)]
    up = [(p, (p + 1) % count) for p in range(count)]
    evens, odds = exchange_pairs(chips, 0), exchange_pairs(chips, 1)
    square, row = (width, width), (1, width)

    def move(value, pairs):
        return lax.ppermute(value, AXES, pairs)

    def exchange(even, odd):
        return move(even, evens), move(odd, odds)

    cm, sent = local_call(
        start_body,
        [square, (4, width)],
        rhs.reshape(row),
        diagonal.reshape(row),
        pattern,
        coupling,
        hbm=4,
        scratch=[
            vmem(*row),
            vmem(*row),
            vmem(*pattern.shape, dtype=pattern.dtype),
            vmem(*square),
            pltpu.SemaphoreType.DMA((4,)),
        ],
    )
    from_inner = move(sent, inner)
    even, odd, scale, state = local_call(
        pair_body, [(2, width), (2, width), (2, width), (4, width)], sent, from_inner
    )
    goteven, gotodd = exchange(even, odd)
    packed, fmat = local_call(
        setup_body,
        [(2 * width + coarse, width), (2 * coarse, 2 * coarse)],
        self_raw,
        coarse_raw,
        coarse_diagonal.reshape(1, 2 * coarse),
        prolong,
        sent,
        cm,
        hbm=4,
        scratch=[
            vmem(*square),
            vmem(2 * coarse, 2 * coarse),
            vmem(1, 2 * coarse),
            vmem(width, coarse),
            pltpu.SemaphoreType.DMA((4,)),
        ],
        flops=100_000_000,
    )
    other = move(packed, inner)
    cm_up = move(cm, up)
    cm_swapped = move(cm_up, inner)
    sl, sr, cin, cint, cr, crt, ptl, ptr, prl, prr = local_call(
        order_body, [square] * 6 + [(coarse, width)] * 2 + [(width, coarse)] * 2, packed, other
    )
    cl, clt = local_call(left_edge_body, [square, square], cm_up, cm_swapped)

    owns = []
    for cycle in range(3):
        if cycle == 0:
            half, even, odd, outer = local_call(
                first_body,
                [(4, width), (2, width), (2, width), (2, width)],
                *(goteven, gotodd, state, scale, fmat),
                *(sl, sr, cin, cint, cr, ptl, ptr, prl, prr),
            )
        else:
            local = local_call(
                restrict_local_body, [(1, 2 * coarse)], state, sl, sr, cin, cint, prl, prr
            )[0]
            half, even, odd = local_call(
                next_body,
                [(4, width), (2, width), (2, width)],
                *(goteven, gotodd, local, state, scale, fmat),
                *(sl, sr, cin, cint, cl, cr, ptl, ptr, prl, prr),
            )
        goteven, gotodd = exchange(even, odd)
        owed = local_call(edge_local_body, [(2, width)], half, outer, clt, crt)[0]
        state, even, odd, own = local_call(
            apply_body,
            [(4, width), row, row, (2, width)],
            *(goteven, gotodd, half, owed, scale, sl, sr, cin, cint, cl, cr),
        )
        owns.append(own)
        if cycle < 2:
            goteven, gotodd = exchange(even, odd)

    parts = local_call(
        gram_body, [(count, LANES)], sent, *owns, scratch=[vmem(3 * GROUP, width)] * 2
    )[0]
    sums = lax.all_to_all(parts, AXES, 0, 0, tiled=True)
    sums = jnp.pad(sums, ((0, -count % 8), (0, 0)))
    sol, res, norms = local_call(finish_body, [row, row, (1, 3)], sums, sent, *owns)
    return sol.reshape(width), res.reshape(width), norms.reshape(3)


def solution(mesh):
    assert mesh.shape["sub"] == 2
    both = P(AXES)
    wide = P(AXES, None)
    return jax.shard_map(
        per_device,
        mesh=mesh,
        in_specs=(both, both, wide, wide, wide, wide, P("dom", None), P("dom")),
        out_specs=(both, both, P()),
        check_vma=False,
    )
```
